32 devices in a mesh: ens: 4 (over z), replica: 2 (over x), model: 4 (over y, core).
Axes of the slice: x: 2, y: 2, z: 4, core: 2. Of those that a mesh axis runs over, the one named last changes fastest.
Arguments:
- slope_up: float32 [8, 768, 3072], P(('ens', 'replica'), None, 'model'), parts along dimension 0, may hold values from -0.875 to 0.875
- slope_down: float32 [8, 3072, 768], P(('ens', 'replica'), 'model'), parts along dimension 0, may hold values from -0.875 to 0.875
- slope_norm: float32 [8, 768], P(('ens', 'replica')), parts along dimension 0, may hold values from -8 to 8
- slope_bias: float32 [8, 768], P(('ens', 'replica')), parts along dimension 0, may hold values from -8 to 8
- param_up: float32 [3072, 3072], P(('ens', 'replica'), 'model'), parts along dimension 0, may hold values from -0.3125 to 0.3125
- param_down: float32 [12288, 768], P(('ens', 'model'), 'replica'), parts along dimension 0, may hold values from -0.15625 to 0.15625
- param_norm: float32 [3072], P(('ens', 'replica')), parts along dimension 0, may hold values from 0.25 to 1.75
- param_bias: float32 [3072], P(('ens', 'replica')), parts along dimension 0, may hold values from -3 to 3
Outputs:
- half_up: bfloat16 [3072, 3072], P('ens', 'model'), parts along dimension 0
- half_down: bfloat16 [12288, 768], P(('ens', 'model')), parts along dimension 0
- half_norm: bfloat16 [3072], P('ens'), parts along dimension 0
- half_bias: bfloat16 [3072], P('ens'), parts along dimension 0
- next_up: float32 [3072, 3072], P(('ens', 'replica'), 'model'), parts along dimension 0
- next_down: float32 [12288, 768], P(('ens', 'model'), 'replica'), parts along dimension 0
- next_norm: float32 [3072], P(('ens', 'replica')), parts along dimension 0
- next_bias: float32 [3072], P(('ens', 'replica')), parts along dimension 0
The draws below stay inside these ranges and needn't reach their ends.
There are 4 independent parts, one for each index of `ens`. The reference program is written for one: setup_inputs(seed, part) draws one part's arguments, and reference() takes and returns one part's arrays. A program takes and returns all parts, laid end to end along the dimension named above; each array names one. Nothing has to cross between parts.
All inputs are finite; a program needn't handle non-finite values.
Results may differ from the reference program's by a relative error of at most 0.0004.
Values may be sent and summed in bfloat16 or wider, within the bound.
A program may use at most 64 MiB of HBM per device.

```python
import jax
import jax.numpy as jnp
from jax import lax

WIDTH = 768
INNER = 3072
REPLICAS = 2


def with_spikes(values, own_key, source, target, parts, factor):
    def block_of(dim):
        return (jnp.arange(values.shape[dim]) // (values.shape[dim] // parts)).reshape((-1,) + (1,) * (values.ndim - 1 - dim))

    one_side = jax.random.permutation(own_key, parts)[block_of(target)]
    second = (block_of(target) + parts // 2) % parts
    return jnp.where((block_of(source) == one_side) | (block_of(source) == second), factor * values, values)


def block_scale(key, extent, split, smallest, largest):
    factor_of, own = 1.0, jax.random.fold_in(key, 6)
    for axis_at, parts in split:
        heights = jnp.exp(jax.random.uniform(jax.random.fold_in(own, axis_at), (parts,), jnp.float32, smallest / len(split), largest / len(split)))
        factor_of = factor_of * jnp.repeat(heights, extent[axis_at] // parts).reshape([-1 if axis == axis_at else 1 for axis in range(len(extent))])
    return factor_of


def gaussian(key, shape, width, most, cuts=(), dtype=jnp.bfloat16):
    factor_of = block_scale(key, shape, cuts, -0.22, 0.18) if cuts else 1.0
    result = jax.random.normal(key, shape, jnp.float32) * width * factor_of
    return jnp.minimum(jnp.maximum(result, -most), most).astype(dtype)


def bell_draw_with(own_key, extent, deviation, reach, cuts, heavy, dtype=jnp.bfloat16):
    result = deviation * jax.random.normal(own_key, extent, jnp.float32)
    if cuts:
        result = result * block_scale(own_key, extent, cuts, -0.22, 0.18)
    return jnp.clip(with_spikes(result, jax.random.fold_in(own_key, 3), *heavy), -reach, reach).astype(dtype)


def setup_inputs(seed: int = 0, part: int = 0) -> dict:
    splits = jax.random.split(jax.random.key(seed), 9)
    own_keys = jax.random.split(jax.random.fold_in(splits[8], part), 9)
    return {
        "slope_up": bell_draw_with(own_keys[0], (REPLICAS, WIDTH, INNER), 0.1, 0.875, ((0, 2), (2, 4)), (0, 1, 2, 2.0), jnp.float32),
        "slope_down": bell_draw_with(own_keys[1], (REPLICAS, INNER, WIDTH), 0.1, 0.875, ((0, 2), (1, 4)), (0, 2, 2, 2.0), jnp.float32),
        "slope_norm": bell_draw_with(own_keys[2], (REPLICAS, WIDTH), 1.0, 8.0, ((0, 2),), (0, 1, 2, 2.0), jnp.float32),
        "slope_bias": bell_draw_with(own_keys[3], (REPLICAS, WIDTH), 1.0, 8.0, ((0, 2),), (0, 1, 2, 2.0), jnp.float32),
        "param_up": bell_draw_with(own_keys[4], (WIDTH, INNER), WIDTH ** -0.5, 0.3125, ((0, 2), (1, 4)), (1, 0, 4, 2.0), jnp.float32),
        "param_down": bell_draw_with(own_keys[5], (INNER, WIDTH), INNER ** -0.5, 0.15625, ((0, 4), (1, 2)), (0, 1, 4, 2.0), jnp.float32),
        "param_norm": jnp.clip(1.0 + 0.15 * jax.random.normal(own_keys[6], (WIDTH,), jnp.float32), 0.25, 1.75),
        "param_bias": gaussian(own_keys[7], (WIDTH,), 0.5, 3.0, ((0, 2),), jnp.float32),
    }


learn_rate = 0.4

def reference(slope_up, slope_down, slope_norm, slope_bias, param_up, param_down, param_norm, param_bias):
    mean_up = lax.optimization_barrier(jnp.sum(slope_up.astype(jnp.float32), axis=0)) * REPLICAS ** (-0.5)
    mean_down = lax.optimization_barrier(jnp.sum(slope_down.astype(jnp.float32), axis=0)) * REPLICAS ** (-0.5)
    mean_norm = lax.optimization_barrier(jnp.sum(slope_norm.astype(jnp.float32), axis=0)) * REPLICAS ** (-0.5)
    mean_bias = lax.optimization_barrier(jnp.sum(slope_bias.astype(jnp.float32), axis=0)) * REPLICAS ** (-0.5)
    ratio_up = jnp.sqrt(lax.optimization_barrier(jnp.sum(param_up * param_up, axis=1, keepdims=True))) * lax.rsqrt(lax.optimization_barrier(jnp.sum(mean_up * mean_up, axis=1, keepdims=True)) + 1e-06)
    mean_up = mean_up * ratio_up
    ratio_down = jnp.sqrt(lax.optimization_barrier(jnp.sum(param_down * param_down, axis=0, keepdims=True))) * lax.rsqrt(lax.optimization_barrier(jnp.sum(mean_down * mean_down, axis=0, keepdims=True)) + 1e-06)
    mean_down = mean_down * ratio_down
    next_up = param_up - learn_rate * mean_up
    next_down = param_down - learn_rate * mean_down
    next_norm = param_norm - learn_rate * mean_norm
    next_bias = param_bias - learn_rate * mean_bias
    half_up = next_up.astype(jnp.bfloat16)
    half_down = next_down.astype(jnp.bfloat16)
    half_norm = next_norm.astype(jnp.bfloat16)
    half_bias = next_bias.astype(jnp.bfloat16)
    return (half_up, half_down, half_norm, half_bias, next_up, next_down, next_norm, next_bias)
```

```python
import functools
import math

import jax
import jax.numpy as jnp
from jax import lax
from jax.experimental import pallas as pl
from jax.experimental.pallas import tpu as pltpu
from jax.sharding import PartitionSpec as P

learn_rate = 0.4
LANES = 128
SPAN = 251.0
MESH = pl.DeviceIdType.MESH


def plain(
    slope_up, slope_down, slope_norm, slope_bias, param_up, param_down, param_norm, param_bias
):
    mean_up, mean_down = (
        lax.psum_scatter(slope_up[0], "replica", scatter_dimension=0, tiled=True),
        lax.psum_scatter(slope_down[0], "replica", scatter_dimension=1, tiled=True),
    )
    whole_norm, whole_bias = lax.psum((slope_norm[0], slope_bias[0]), "replica")
    place = lax.axis_index("replica")
    mean_norm = lax.dynamic_slice_in_dim(
        whole_norm, place * param_norm.shape[0], param_norm.shape[0]
    )
    mean_bias = lax.dynamic_slice_in_dim(
        whole_bias, place * param_bias.shape[0], param_bias.shape[0]
    )
    mean_rate = lax.axis_size("replica") ** (-0.5)
    mean_up = mean_up * mean_rate
    mean_down = mean_down * mean_rate
    mean_norm = mean_norm * mean_rate
    mean_bias = mean_bias * mean_rate
    own_up, own_down, slope_up_norm, slope_down_norm = lax.psum(
        (
            jnp.sum(param_up * param_up, axis=1, keepdims=True),
            jnp.sum(param_down * param_down, axis=0, keepdims=True),
            jnp.sum(mean_up * mean_up, axis=1, keepdims=True),
            jnp.sum(mean_down * mean_down, axis=0, keepdims=True),
        ),
        "model",
    )
    mean_up = mean_up * (jnp.sqrt(own_up) * lax.rsqrt(slope_up_norm + 1e-06))
    mean_down = mean_down * (jnp.sqrt(own_down) * lax.rsqrt(slope_down_norm + 1e-06))
    next_up = param_up - learn_rate * mean_up
    next_down = param_down - learn_rate * mean_down
    next_norm = param_norm - learn_rate * mean_norm
    next_bias = param_bias - learn_rate * mean_bias
    half_up, half_down, half_norm, half_bias = (
        lax.all_gather(next_up.astype(jnp.bfloat16), "replica", axis=0, tiled=True),
        lax.all_gather(next_down.astype(jnp.bfloat16), "replica", axis=1, tiled=True),
        lax.all_gather(next_norm.astype(jnp.bfloat16), "replica", axis=0, tiled=True),
        lax.all_gather(next_bias.astype(jnp.bfloat16), "replica", axis=0, tiled=True),
    )
    return (half_up, half_down, half_norm, half_bias, next_up, next_down, next_norm, next_bias)


def encode(x, factor):
    size = jnp.exp2(SPAN * jnp.sqrt(jnp.abs(x) * factor) - 125.0)
    return jnp.where(x < 0, -size, size).astype(jnp.bfloat16)


def decode(y, most):
    y = y.astype(jnp.float32)
    u = jnp.log(jnp.abs(y)) * (math.log2(math.e) / SPAN) + 125.0 / SPAN
    size = u * u * most
    return jnp.where(y < 0, -size, size)


def kernel(
    models,
    s_up, s_down, s_norm, s_bias, p_up, p_down, p_norm, p_bias,
    half_up, half_down, new_up, new_down, h_norm, h_bias, n_norm, n_bias,
    far, near, param, code, got, scale, got_scale, stat, got_stat, mine, theirs,
    far_sem, near_sem, param_sem, vec_sem,
    code_send, code_recv, scale_send, scale_recv, stat_send, stat_recv,
    half_send, half_recv, vec_send, vec_recv,
):
    me, model = lax.axis_index("replica"), lax.axis_index("model")
    other = 1 - me
    share = p_up.shape[0]
    blocks = p_up.shape[1] // LANES
    per = share // LANES
    chunks = 2 * per
    rate = lax.axis_size("replica") ** (-0.5)

    def at(start):
        return pl.ds(pl.multiple_of(start, LANES), LANES)

    def is_up(c):
        return c >= per

    def slope_at(c, who):
        if is_up(c):
            return s_up.at[0, at(who * share + (c - per) * LANES), :]
        return s_down.at[0, :, at(who * share + c * LANES)]

    def own_at(c, up, down):
        if is_up(c):
            return up.at[pl.ds((c - per) * LANES, LANES), :]
        return down.at[:, pl.ds(c * LANES, LANES)]

    def buf(bufs, c):
        return bufs[0].at[c - per] if is_up(c) else bufs[1].at[c]

    def block(bufs, c, k):
        if is_up(c):
            return bufs[0].at[c - per, :, pl.ds(k * LANES, LANES)]
        return bufs[1].at[c, pl.ds(k * LANES, LANES), :]

    def to_row(c, x, fold):
        return fold(x.T if is_up(c) else x, axis=0, keepdims=True)

    def to_block(c, row):
        x = jnp.broadcast_to(row, (LANES, LANES))
        return x.T if is_up(c) else x

    far_load = [pltpu.make_async_copy(slope_at(c, other), buf(far, c), far_sem.at[c]) for c in range(chunks)]
    near_load = [pltpu.make_async_copy(slope_at(c, me), buf(near, c), near_sem.at[c]) for c in range(chunks)]
    param_load = [
        pltpu.make_async_copy(own_at(c, p_up, p_down), buf(param, c), param_sem.at[c])
        for c in range(chunks)
    ]
    new = (new_up, new_down)
    half = (half_up.at[me], half_down.at[me])

    def remote(src, dst, send, recv, where):
        return pltpu.make_async_remote_copy(
            src_ref=src, dst_ref=dst, send_sem=send, recv_sem=recv,
            device_id=where, device_id_type=MESH,
        )

    partner = {"replica": other}
    peers = [{"model": lax.rem(model + d, models)} for d in range(1, models)]
    barrier = pltpu.get_barrier_semaphore()
    for where in [partner] + peers:
        pl.semaphore_signal(barrier, inc=1, device_id=where, device_id_type=MESH)
    for copy in far_load[:2]:
        copy.start()

    code_copy = [remote(buf(code, c), buf(got, c), code_send.at[c], code_recv.at[c], partner) for c in range(chunks)]
    scale_copy = [remote(scale.at[c], got_scale.at[c], scale_send.at[c], scale_recv.at[c], partner) for c in range(chunks)]
    stat_copy = [
        [
            remote(stat.at[c], got_stat.at[c, d], stat_send.at[c, d], stat_recv.at[c, d], where)
            for d, where in enumerate(peers)
        ]
        for c in range(chunks)
    ]
    half_copy = [remote(buf(half, c), buf(half, c), half_send.at[c], half_recv.at[c], partner) for c in range(chunks)]
    vectors = (s_norm, s_bias, p_norm, p_bias)
    vec_load = [pltpu.make_async_copy(src, mine[i], vec_sem.at[i]) for i, src in enumerate(vectors)]
    vec_copy = [
        remote(src, theirs[i], vec_send.at[i], vec_recv.at[i], partner)
        for i, src in enumerate(vectors)
    ]

    for c in range(chunks):
        far_load[c].wait()
        if c + 2 < chunks:
            far_load[c + 2].start()
        top = jnp.zeros((LANES, LANES), jnp.float32)
        for k in range(blocks):
            top = jnp.maximum(top, jnp.abs(block(far, c, k)[...]))
        most = jnp.maximum(to_row(c, top, jnp.max), 1e-30)
        scale[c] = most
        factor = to_block(c, 1.0 / most)
        for k in range(blocks):
            block(code, c, k)[...] = encode(block(far, c, k)[...], factor)
        if c == 0:
            pl.semaphore_wait(barrier, models)
        scale_copy[c].start()
        code_copy[c].start()
        if c == 0:
            for copy in vec_copy + vec_load:
                copy.start()
        near_load[c].start()
        param_load[c].start()

    def reduce(c):
        near_load[c].wait()
        param_load[c].wait()
        scale_copy[c].wait_recv()
        code_copy[c].wait_recv()
        factor = to_block(c, got_scale[c])
        own = jnp.zeros((LANES, LANES), jnp.float32)
        slope = jnp.zeros((LANES, LANES), jnp.float32)
        for k in range(blocks):
            mean = (block(near, c, k)[...] + decode(block(got, c, k)[...], factor)) * rate
            block(near, c, k)[...] = mean
            slope = slope + mean * mean
            p = block(param, c, k)[...]
            own = own + p * p
        stat[c, 0:1, :] = to_row(c, own, jnp.sum)
        stat[c, 1:2, :] = to_row(c, slope, jnp.sum)
        for copy in stat_copy[c]:
            copy.start()

    def update(c):
        total = stat[c, 0:2, :]
        for d in range(models - 1):
            stat_copy[c][d].wait_recv()
            total = total + got_stat[c, d, 0:2, :]
        ratio = to_block(c, jnp.sqrt(total[0:1]) * lax.rsqrt(total[1:2] + 1e-06))
        for k in range(blocks):
            fresh = block(param, c, k)[...] - learn_rate * (block(near, c, k)[...] * ratio)
            block(new, c, k)[...] = fresh
            block(half, c, k)[...] = fresh.astype(jnp.bfloat16)
        half_copy[c].start()

    for c in range(chunks):
        reduce(c)
        if c > 0:
            update(c - 1)
    update(chunks - 1)

    def vector(i, h, n):
        for copy in (vec_load[i], vec_load[i + 2], vec_copy[i], vec_copy[i + 2]):
            copy.wait()
        mean = (mine[i][0, :] + theirs[i][0, :]) * rate
        here, there = mine[i + 2][...], theirs[i + 2][...]
        low = jnp.where(me == 0, here, there) - learn_rate * mean[:share]
        high = jnp.where(me == 0, there, here) - learn_rate * mean[share:]
        h[...] = jnp.concatenate([low, high]).astype(jnp.bfloat16)
        n[...] = jnp.where(me == 0, low, high)

    vector(0, h_norm, n_norm)
    vector(1, h_bias, n_bias)
    for c in range(chunks):
        scale_copy[c].wait_send()
        code_copy[c].wait_send()
        for copy in stat_copy[c]:
            copy.wait_send()
        half_copy[c].wait()


def store(
    half_up, half_down, new_up, new_down, k_norm, k_bias, m_norm, m_bias,
    h_up, h_down, h_norm, h_bias, n_up, n_down, n_norm, n_bias, sem,
):
    replicas, per = half_up.shape[:2]
    share = per * LANES
    copies = []

    def put(src, dst):
        copy = pltpu.make_async_copy(src, dst, sem.at[len(copies)])
        copy.start()
        copies.append(copy)

    for c in range(per):
        part = pl.ds(c * LANES, LANES)
        put(new_up.at[c], n_up.at[part, :])
        put(new_down.at[c], n_down.at[:, part])
        for who in range(replicas):
            part = pl.ds(who * share + c * LANES, LANES)
            put(half_up.at[who, c], h_up.at[part, :])
            put(half_down.at[who, c], h_down.at[:, part])
    for src, dst in ((k_norm, h_norm), (k_bias, h_bias), (m_norm, n_norm), (m_bias, n_bias)):
        put(src, dst)
    for copy in copies:
        copy.wait()


def fused(mesh, s_up, s_down, s_norm, s_bias, p_up, p_down, p_norm, p_bias):
    models, replicas = mesh.shape["model"], mesh.shape["replica"]
    width, inner = s_up.shape[1:]
    share = p_up.shape[0]
    per = share // LANES
    chunks = 2 * per
    f32, bf16 = jnp.float32, jnp.bfloat16
    any_spec = pl.BlockSpec(memory_space=pl.ANY)
    vmem = pl.BlockSpec(memory_space=pltpu.VMEM)
    hbm = pl.BlockSpec(memory_space=pltpu.HBM)
    dma = pltpu.SemaphoreType.DMA

    def pair(dtype):
        return (pltpu.VMEM((per, LANES, inner), dtype), pltpu.VMEM((per, inner, LANES), dtype))

    vecs = (
        pltpu.VMEM((1, width), f32), pltpu.VMEM((1, width), f32),
        pltpu.VMEM((share,), f32), pltpu.VMEM((share,), f32),
    )
    shape = jax.ShapeDtypeStruct
    held = pl.pallas_call(
        functools.partial(kernel, models),
        out_shape=(
            pltpu.VMEM((replicas, per, LANES, inner), bf16),
            pltpu.VMEM((replicas, per, inner, LANES), bf16),
            *pair(f32),
            pltpu.VMEM((width,), bf16),
            pltpu.VMEM((width,), bf16),
            pltpu.VMEM((share,), f32),
            pltpu.VMEM((share,), f32),
        ),
        in_specs=[hbm] * 8,
        out_specs=[vmem] * 8,
        scratch_shapes=[
            pair(f32), pair(f32), pair(f32), pair(bf16), pair(bf16),
            pltpu.VMEM((chunks, 1, LANES), f32), pltpu.VMEM((chunks, 1, LANES), f32),
            pltpu.VMEM((chunks, 8, LANES), f32), pltpu.VMEM((chunks, models - 1, 8, LANES), f32),
            vecs, vecs,
            dma((chunks,)), dma((chunks,)), dma((chunks,)), dma((4,)),
            dma((chunks,)), dma((chunks,)), dma((chunks,)), dma((chunks,)),
            dma((chunks, models - 1)), dma((chunks, models - 1)),
            dma((chunks,)), dma((chunks,)), dma((4,)), dma((4,)),
        ],
        compiler_params=pltpu.CompilerParams(
            collective_id=0, has_side_effects=True, vmem_limit_bytes=58 * 2**20
        ),
    )(s_up, s_down, s_norm, s_bias, p_up, p_down, p_norm, p_bias)
    return pl.pallas_call(
        store,
        out_shape=(
            shape((width, inner), bf16),
            shape((inner, width), bf16),
            shape((width,), bf16),
            shape((width,), bf16),
            shape((share, inner), f32),
            shape((inner, share), f32),
            shape((share,), f32),
            shape((share,), f32),
        ),
        in_specs=[vmem] * 8,
        out_specs=[any_spec] * 8,
        scratch_shapes=[dma(((2 + 2 * replicas) * per + 4,))],
        compiler_params=pltpu.CompilerParams(
            has_side_effects=True, vmem_limit_bytes=16 * 2**20
        ),
    )(*held)


def solution(mesh):
    in_specs = (
        P(("ens", "replica"), None, "model"),
        P(("ens", "replica"), "model", None),
        P(("ens", "replica"), None),
        P(("ens", "replica"), None),
        P(("ens", "replica"), "model"),
        P(("ens", "model"), "replica"),
        P(("ens", "replica")),
        P(("ens", "replica")),
    )
    out_specs = (
        P("ens", "model"),
        P(("ens", "model"), None),
        P("ens"),
        P("ens"),
        P(("ens", "replica"), "model"),
        P(("ens", "model"), "replica"),
        P(("ens", "replica")),
        P(("ens", "replica")),
    )

    def on_device(*args):
        share, inner = args[4].shape
        if mesh.shape["replica"] == 2 and share % LANES == 0 and inner % LANES == 0:
            return fused(mesh, *args)
        return plain(*args)

    return jax.shard_map(
        on_device, mesh=mesh, in_specs=in_specs, out_specs=out_specs, check_vma=False
    )
```

```python
import functools
import math

import jax
import jax.numpy as jnp
from jax import lax
from jax.experimental import pallas as pl
from jax.experimental.pallas import tpu as pltpu
from jax.sharding import PartitionSpec as P

learn_rate = 0.4
LANES = 128
SPAN = 251.0
MESH = pl.DeviceIdType.MESH


def plain(
    slope_up, slope_down, slope_norm, slope_bias, param_up, param_down, param_norm, param_bias
):
    mean_up, mean_down = (
        lax.psum_scatter(slope_up[0], "replica", scatter_dimension=0, tiled=True),
        lax.psum_scatter(slope_down[0], "replica", scatter_dimension=1, tiled=True),
    )
    whole_norm, whole_bias = lax.psum((slope_norm[0], slope_bias[0]), "replica")
    place = lax.axis_index("replica")
    mean_norm = lax.dynamic_slice_in_dim(
        whole_norm, place * param_norm.shape[0], param_norm.shape[0]
    )
    mean_bias = lax.dynamic_slice_in_dim(
        whole_bias, place * param_bias.shape[0], param_bias.shape[0]
    )
    mean_rate = lax.axis_size("replica") ** (-0.5)
    mean_up = mean_up * mean_rate
    mean_down = mean_down * mean_rate
    mean_norm = mean_norm * mean_rate
    mean_bias = mean_bias * mean_rate
    own_up, own_down, slope_up_norm, slope_down_norm = lax.psum(
        (
            jnp.sum(param_up * param_up, axis=1, keepdims=True),
            jnp.sum(param_down * param_down, axis=0, keepdims=True),
            jnp.sum(mean_up * mean_up, axis=1, keepdims=True),
            jnp.sum(mean_down * mean_down, axis=0, keepdims=True),
        ),
        "model",
    )
    mean_up = mean_up * (jnp.sqrt(own_up) * lax.rsqrt(slope_up_norm + 1e-06))
    mean_down = mean_down * (jnp.sqrt(own_down) * lax.rsqrt(slope_down_norm + 1e-06))
    next_up = param_up - learn_rate * mean_up
    next_down = param_down - learn_rate * mean_down
    next_norm = param_norm - learn_rate * mean_norm
    next_bias = param_bias - learn_rate * mean_bias
    half_up, half_down, half_norm, half_bias = (
        lax.all_gather(next_up.astype(jnp.bfloat16), "replica", axis=0, tiled=True),
        lax.all_gather(next_down.astype(jnp.bfloat16), "replica", axis=1, tiled=True),
        lax.all_gather(next_norm.astype(jnp.bfloat16), "replica", axis=0, tiled=True),
        lax.all_gather(next_bias.astype(jnp.bfloat16), "replica", axis=0, tiled=True),
    )
    return (half_up, half_down, half_norm, half_bias, next_up, next_down, next_norm, next_bias)


def encode(x, factor):
    size = jnp.exp2(SPAN * jnp.sqrt(jnp.abs(x) * factor) - 125.0)
    return jnp.where(x < 0, -size, size).astype(jnp.bfloat16)


def decode(y, most):
    y = y.astype(jnp.float32)
    u = jnp.log(jnp.abs(y)) * (math.log2(math.e) / SPAN) + 125.0 / SPAN
    size = u * u * most
    return jnp.where(y < 0, -size, size)


def kernel(
    models,
    s_up, s_down, s_norm, s_bias, p_up, p_down, p_norm, p_bias,
    half_up, half_down, new_up, new_down, h_norm, h_bias, n_norm, n_bias,
    far, near, param, code, got, scale, got_scale, stat, got_stat, mine, theirs, ready,
    far_sem, near_sem, param_sem, vec_sem,
    code_send, code_recv, scale_send, scale_recv, stat_send, stat_recv,
    half_send, half_recv, vec_send, vec_recv,
):
    me, model = lax.axis_index("replica"), lax.axis_index("model")
    other = 1 - me
    share = p_up.shape[0]
    blocks = p_up.shape[1] // LANES
    per = share // LANES
    chunks = 2 * per
    rate = lax.axis_size("replica") ** (-0.5)

    def at(start):
        return pl.ds(pl.multiple_of(start, LANES), LANES)

    def is_up(c):
        return c >= per

    def slope_at(c, who):
        if is_up(c):
            return s_up.at[0, at(who * share + (c - per) * LANES), :]
        return s_down.at[0, :, at(who * share + c * LANES)]

    def own_at(c, up, down):
        if is_up(c):
            return up.at[pl.ds((c - per) * LANES, LANES), :]
        return down.at[:, pl.ds(c * LANES, LANES)]

    def buf(bufs, c):
        return bufs[0].at[c - per] if is_up(c) else bufs[1].at[c]

    def block(bufs, c, k):
        if is_up(c):
            return bufs[0].at[c - per, :, pl.ds(k * LANES, LANES)]
        return bufs[1].at[c, pl.ds(k * LANES, LANES), :]

    def to_row(c, x, fold):
        return fold(x.T if is_up(c) else x, axis=0, keepdims=True)

    def to_block(c, row):
        x = jnp.broadcast_to(row, (LANES, LANES))
        return x.T if is_up(c) else x

    far_load = [pltpu.make_async_copy(slope_at(c, other), buf(far, c), far_sem.at[c]) for c in range(chunks)]
    near_load = [pltpu.make_async_copy(slope_at(c, me), buf(near, c), near_sem.at[c]) for c in range(chunks)]
    param_load = [
        pltpu.make_async_copy(own_at(c, p_up, p_down), buf(param, c), param_sem.at[c])
        for c in range(chunks)
    ]
    new = (new_up, new_down)
    half = (half_up.at[me], half_down.at[me])

    def remote(src, dst, send, recv, where):
        return pltpu.make_async_remote_copy(
            src_ref=src, dst_ref=dst, send_sem=send, recv_sem=recv,
            device_id=where, device_id_type=MESH,
        )

    partner = {"replica": other}
    peers = [{"model": lax.rem(model + d, models)} for d in range(1, models)]
    barrier = pltpu.get_barrier_semaphore()

    def signal(sem, where):
        pl.semaphore_signal(sem, inc=1, device_id=where, device_id_type=MESH)

    @pl.when(me == 0)
    def _():
        signal(barrier, partner)

    for copy in far_load[:2]:
        copy.start()

    @pl.when(me == 1)
    def _():
        pl.semaphore_wait(barrier, 1)
        signal(ready, partner)

    def meet_partner():
        @pl.when(me == 0)
        def _():
            pl.semaphore_wait(ready, 1)
            for where in peers:
                signal(barrier, where)

    def meet_peers():
        @pl.when(me == 0)
        def _():
            pl.semaphore_wait(barrier, models - 1)
            signal(ready, partner)

        @pl.when(me == 1)
        def _():
            pl.semaphore_wait(ready, 1)

    code_copy = [remote(buf(code, c), buf(got, c), code_send.at[c], code_recv.at[c], partner) for c in range(chunks)]
    scale_copy = [remote(scale.at[c], got_scale.at[c], scale_send.at[c], scale_recv.at[c], partner) for c in range(chunks)]
    stat_copy = [
        [
            remote(stat.at[c], got_stat.at[c, d], stat_send.at[c, d], stat_recv.at[c, d], where)
            for d, where in enumerate(peers)
        ]
        for c in range(chunks)
    ]
    half_copy = [remote(buf(half, c), buf(half, c), half_send.at[c], half_recv.at[c], partner) for c in range(chunks)]
    vectors = (s_norm, s_bias, p_norm, p_bias)
    vec_load = [pltpu.make_async_copy(src, mine[i], vec_sem.at[i]) for i, src in enumerate(vectors)]
    vec_copy = [
        remote(src, theirs[i], vec_send.at[i], vec_recv.at[i], partner)
        for i, src in enumerate(vectors)
    ]

    for c in range(chunks):
        far_load[c].wait()
        if c + 2 < chunks:
            far_load[c + 2].start()
        top = jnp.zeros((LANES, LANES), jnp.float32)
        for k in range(blocks):
            top = jnp.maximum(top, jnp.abs(block(far, c, k)[...]))
        most = jnp.maximum(to_row(c, top, jnp.max), 1e-30)
        scale[c] = most
        factor = to_block(c, 1.0 / most)
        for k in range(blocks):
            block(code, c, k)[...] = encode(block(far, c, k)[...], factor)
        if c == 0:
            meet_partner()
        scale_copy[c].start()
        code_copy[c].start()
        if c == 0:
            for copy in vec_copy + vec_load:
                copy.start()
        near_load[c].start()
        param_load[c].start()

    meet_peers()

    def reduce(c):
        near_load[c].wait()
        param_load[c].wait()
        scale_copy[c].wait_recv()
        code_copy[c].wait_recv()
        factor = to_block(c, got_scale[c])
        own = jnp.zeros((LANES, LANES), jnp.float32)
        slope = jnp.zeros((LANES, LANES), jnp.float32)
        for k in range(blocks):
            mean = (block(near, c, k)[...] + decode(block(got, c, k)[...], factor)) * rate
            block(near, c, k)[...] = mean
            slope = slope + mean * mean
            p = block(param, c, k)[...]
            own = own + p * p
        stat[c, 0:1, :] = to_row(c, own, jnp.sum)
        stat[c, 1:2, :] = to_row(c, slope, jnp.sum)
        for copy in stat_copy[c]:
            copy.start()

    def update(c):
        total = stat[c, 0:2, :]
        for d in range(models - 1):
            stat_copy[c][d].wait_recv()
            total = total + got_stat[c, d, 0:2, :]
        ratio = to_block(c, jnp.sqrt(total[0:1]) * lax.rsqrt(total[1:2] + 1e-06))
        for k in range(blocks):
            fresh = block(param, c, k)[...] - learn_rate * (block(near, c, k)[...] * ratio)
            block(new, c, k)[...] = fresh
            block(half, c, k)[...] = fresh.astype(jnp.bfloat16)
        half_copy[c].start()

    for c in range(chunks):
        reduce(c)
        if c > 0:
            update(c - 1)
    update(chunks - 1)

    def vector(i, h, n):
        for copy in (vec_load[i], vec_load[i + 2], vec_copy[i], vec_copy[i + 2]):
            copy.wait()
        mean = (mine[i][0, :] + theirs[i][0, :]) * rate
        here, there = mine[i + 2][...], theirs[i + 2][...]
        low = jnp.where(me == 0, here, there) - learn_rate * mean[:share]
        high = jnp.where(me == 0, there, here) - learn_rate * mean[share:]
        h[...] = jnp.concatenate([low, high]).astype(jnp.bfloat16)
        n[...] = jnp.where(me == 0, low, high)

    vector(0, h_norm, n_norm)
    vector(1, h_bias, n_bias)
    for c in range(chunks):
        scale_copy[c].wait_send()
        code_copy[c].wait_send()
        for copy in stat_copy[c]:
            copy.wait_send()
        half_copy[c].wait()


def store(
    half_up, half_down, new_up, new_down, k_norm, k_bias, m_norm, m_bias,
    h_up, h_down, h_norm, h_bias, n_up, n_down, n_norm, n_bias, sem,
):
    replicas, per = half_up.shape[:2]
    share = per * LANES
    copies = []

    def put(src, dst):
        copy = pltpu.make_async_copy(src, dst, sem.at[len(copies)])
        copy.start()
        copies.append(copy)

    for c in range(per):
        part = pl.ds(c * LANES, LANES)
        put(new_up.at[c], n_up.at[part, :])
        put(new_down.at[c], n_down.at[:, part])
        for who in range(replicas):
            part = pl.ds(who * share + c * LANES, LANES)
            put(half_up.at[who, c], h_up.at[part, :])
            put(half_down.at[who, c], h_down.at[:, part])
    for src, dst in ((k_norm, h_norm), (k_bias, h_bias), (m_norm, n_norm), (m_bias, n_bias)):
        put(src, dst)
    for copy in copies:
        copy.wait()


def fused(mesh, s_up, s_down, s_norm, s_bias, p_up, p_down, p_norm, p_bias):
    models, replicas = mesh.shape["model"], mesh.shape["replica"]
    width, inner = s_up.shape[1:]
    share = p_up.shape[0]
    per = share // LANES
    chunks = 2 * per
    f32, bf16 = jnp.float32, jnp.bfloat16
    any_spec = pl.BlockSpec(memory_space=pl.ANY)
    vmem = pl.BlockSpec(memory_space=pltpu.VMEM)
    hbm = pl.BlockSpec(memory_space=pltpu.HBM)
    dma = pltpu.SemaphoreType.DMA

    def pair(dtype):
        return (pltpu.VMEM((per, LANES, inner), dtype), pltpu.VMEM((per, inner, LANES), dtype))

    vecs = (
        pltpu.VMEM((1, width), f32), pltpu.VMEM((1, width), f32),
        pltpu.VMEM((share,), f32), pltpu.VMEM((share,), f32),
    )
    shape = jax.ShapeDtypeStruct
    held = pl.pallas_call(
        functools.partial(kernel, models),
        out_shape=(
            pltpu.VMEM((replicas, per, LANES, inner), bf16),
            pltpu.VMEM((replicas, per, inner, LANES), bf16),
            *pair(f32),
            pltpu.VMEM((width,), bf16),
            pltpu.VMEM((width,), bf16),
            pltpu.VMEM((share,), f32),
            pltpu.VMEM((share,), f32),
        ),
        in_specs=[hbm] * 8,
        out_specs=[vmem] * 8,
        scratch_shapes=[
            pair(f32), pair(f32), pair(f32), pair(bf16), pair(bf16),
            pltpu.VMEM((chunks, 1, LANES), f32), pltpu.VMEM((chunks, 1, LANES), f32),
            pltpu.VMEM((chunks, 8, LANES), f32), pltpu.VMEM((chunks, models - 1, 8, LANES), f32),
            vecs, vecs, pltpu.SemaphoreType.REGULAR,
            dma((chunks,)), dma((chunks,)), dma((chunks,)), dma((4,)),
            dma((chunks,)), dma((chunks,)), dma((chunks,)), dma((chunks,)),
            dma((chunks, models - 1)), dma((chunks, models - 1)),
            dma((chunks,)), dma((chunks,)), dma((4,)), dma((4,)),
        ],
        compiler_params=pltpu.CompilerParams(
            collective_id=0, has_side_effects=True, vmem_limit_bytes=58 * 2**20
        ),
    )(s_up, s_down, s_norm, s_bias, p_up, p_down, p_norm, p_bias)
    return pl.pallas_call(
        store,
        out_shape=(
            shape((width, inner), bf16),
            shape((inner, width), bf16),
            shape((width,), bf16),
            shape((width,), bf16),
            shape((share, inner), f32),
            shape((inner, share), f32),
            shape((share,), f32),
            shape((share,), f32),
        ),
        in_specs=[vmem] * 8,
        out_specs=[any_spec] * 8,
        scratch_shapes=[dma(((2 + 2 * replicas) * per + 4,))],
        compiler_params=pltpu.CompilerParams(
            has_side_effects=True, vmem_limit_bytes=16 * 2**20
        ),
    )(*held)


def solution(mesh):
    in_specs = (
        P(("ens", "replica"), None, "model"),
        P(("ens", "replica"), "model", None),
        P(("ens", "replica"), None),
        P(("ens", "replica"), None),
        P(("ens", "replica"), "model"),
        P(("ens", "model"), "replica"),
        P(("ens", "replica")),
        P(("ens", "replica")),
    )
    out_specs = (
        P("ens", "model"),
        P(("ens", "model"), None),
        P("ens"),
        P("ens"),
        P(("ens", "replica"), "model"),
        P(("ens", "model"), "replica"),
        P(("ens", "replica")),
        P(("ens", "replica")),
    )

    def on_device(*args):
        share, inner = args[4].shape
        if mesh.shape["replica"] == 2 and share % LANES == 0 and inner % LANES == 0:
            return fused(mesh, *args)
        return plain(*args)

    return jax.shard_map(
        on_device, mesh=mesh, in_specs=in_specs, out_specs=out_specs, check_vma=False
    )
```
